32 devices in a mesh: ta: 4 (over y, core), xyz: 8 (over z, x).
Axes of the slice: x: 2, y: 2, z: 4, core: 2. Of those that a mesh axis runs over, the one named last changes fastest.
Arguments:
- prop_one: bfloat16 [4, 2, 12, 12, 32768], P('ta', None, None, None, 'xyz'), may hold values from -1.796875 to 1.796875
- prop_two: bfloat16 [4, 2, 12, 12, 32768], P('ta', None, None, None, 'xyz'), may hold values from -1.796875 to 1.796875
Outputs:
- momentum_fields: float32 [4, 16, 2, 32768], P(None, 'ta', None, 'xyz')
The draws below stay inside these ranges and needn't reach their ends.
All inputs are finite; a program needn't handle non-finite values.
Results may differ from the reference program's by a relative error of at most 0.0003.
Values sent between devices are 32-bit elements; how exact they have to be, the bound alone decides.
A program may use at most 128 MiB of HBM per device.

```python
import jax
import jax.numpy as jnp
import numpy as np
from jax import lax

L = 32
TIMES = 4
SITES = 32768


def level_of(key, extent, split, low, top_value):
    loudness, own = 1.0, jax.random.fold_in(key, 6)
    for axis_at, parts in split:
        heights = jnp.exp(jax.random.uniform(jax.random.fold_in(own, axis_at), (parts,), jnp.float32, low / len(split), top_value / len(split)))
        loudness = loudness * jnp.repeat(heights, extent[axis_at] // parts).reshape([-1 if axis == axis_at else 1 for axis in range(len(extent))])
    return loudness


def centred(own_key, shape, spread, limit, cuts=(), dtype=jnp.bfloat16):
    factor_of = level_of(own_key, shape, cuts, -0.22, 0.18) if cuts else 1.0
    values = jax.random.normal(own_key, shape, jnp.float32) * spread * factor_of
    return jnp.minimum(jnp.maximum(values, -limit), limit).astype(dtype)


def setup_inputs(seed: int = 0) -> dict:
    seeds = jax.random.split(jax.random.key(seed), 3)
    return {
        "prop_one": centred(seeds[0], (TIMES, 2, 12, 12, SITES), 0.2887, 1.796875, ((0, 4), (4, 8))),
        "prop_two": centred(seeds[1], (TIMES, 2, 12, 12, SITES), 0.2887, 1.796875, ((0, 4), (4, 8))),
    }


spin_columns = [[3, 2, 1, 0], [3, 2, 1, 0], [2, 3, 0, 1], [2, 3, 0, 1]]
spin_phases = [[1j, 1j, -1j, -1j], [-1.0, 1.0, 1.0, -1.0], [1j, -1j, -1j, 1j], [1.0, 1.0, 1.0, 1.0]]
chiral_signs = [1.0, 1.0, -1.0, -1.0]


def vertex_parts():
    result = []
    for gamma_index in range(4):
        columns = spin_columns[gamma_index]
        phases = spin_phases[gamma_index]
        rows_list = [columns[a // 3] * 3 + a % 3 for a in range(12)]
        phase_list = [complex(phases[a // 3]) for a in range(12)]
        result.append((rows_list, phase_list))
    return result, [chiral_signs[a // 3] for a in range(12)]


def build_operands(prop_a, prop_b):
    gammas, chirality = vertex_parts()
    left_real, left_imag, right_real, right_imag = [], [], [], []
    for rows_list, phase_list in gammas:
        pick_real = jnp.stack([prop_a[0, q] for q in rows_list])
        pick_imag = jnp.stack([prop_a[1, q] for q in rows_list])
        phase_real = jnp.asarray(np.array([p.real for p in phase_list]), jnp.bfloat16)[:, None, None]
        phase_imag = jnp.asarray(np.array([p.imag for p in phase_list]), jnp.bfloat16)[:, None, None]
        left_real.append(phase_real * pick_real - phase_imag * pick_imag)
        left_imag.append(phase_real * pick_imag + phase_imag * pick_real)
        col_real = jnp.stack([prop_b[0][:, q] for q in rows_list], axis=1)
        col_imag = jnp.stack([prop_b[1][:, q] for q in rows_list], axis=1)
        factor = np.array([[phase_list[c] * chirality[rows_list[c]] * chirality[a] for c in range(12)] for a in range(12)])
        factor_real = jnp.asarray(factor.real, jnp.bfloat16)[:, :, None]
        factor_imag = jnp.asarray(factor.imag, jnp.bfloat16)[:, :, None]
        right_real.append(factor_real * col_real + factor_imag * col_imag)
        right_imag.append(factor_imag * col_real - factor_real * col_imag)
    left_rows = jnp.stack(left_real + left_imag).reshape(8, 144, -1)
    right_rows = jnp.stack(right_real + right_imag).reshape(8, 144, -1)
    return left_rows, right_rows


def combine_products(products):
    real_sum = products[:4, :4] - products[4:, 4:]
    imag_sum = products[:4, 4:] + products[4:, :4]
    return jnp.stack([real_sum.reshape(16, -1), imag_sum.reshape(16, -1)], axis=1)


def contract(prop_a, prop_b):
    left_rows, right_rows = build_operands(prop_a, prop_b)
    products = jnp.einsum("mks,nks->mns", left_rows.astype(jnp.float32), right_rows.astype(jnp.float32))
    return combine_products(products)


def reference(prop_one, prop_two):
    def per_slice(slice_pair):
        first_planes = jnp.moveaxis(slice_pair[0].reshape(2, 12, 12, L, L * L), 3, 0)
        second_planes = jnp.moveaxis(slice_pair[1].reshape(2, 12, 12, L, L * L), 3, 0)
        fields = lax.map(lambda plane_pair: contract(plane_pair[0], plane_pair[1]), (first_planes, second_planes))
        fields = jnp.moveaxis(fields, 0, 2).reshape(16, 2, L * L * L)
        complex_field = lax.complex(fields[:, 0], fields[:, 1]).reshape(16, L, L, L)
        spectrum = jnp.fft.fftn(complex_field, axes=(1, 2, 3), norm="ortho")
        spectrum = jnp.transpose(spectrum, (0, 2, 3, 1)).reshape(16, L * L * L)
        return jnp.stack([jnp.real(spectrum), jnp.imag(spectrum)], axis=1).astype(jnp.float32)

    return lax.map(per_slice, (prop_one, prop_two))
```

```python
import math

import jax
import jax.numpy as jnp
import numpy as np
from jax import lax
from jax.experimental import pallas as pl
from jax.experimental.pallas import tpu as pltpu
from jax.sharding import PartitionSpec as P

L = 32


spin_columns = [[3, 2, 1, 0], [3, 2, 1, 0], [2, 3, 0, 1], [2, 3, 0, 1]]
spin_phases = [[1j, 1j, -1j, -1j], [-1.0, 1.0, 1.0, -1.0], [1j, -1j, -1j, 1j], [1.0, 1.0, 1.0, 1.0]]
chiral_signs = [1.0, 1.0, -1.0, -1.0]


def vertex_parts():
    result = []
    for gamma_index in range(4):
        columns = spin_columns[gamma_index]
        phases = spin_phases[gamma_index]
        rows_list = [columns[a // 3] * 3 + a % 3 for a in range(12)]
        phase_list = [complex(phases[a // 3]) for a in range(12)]
        result.append((rows_list, phase_list))
    return (result, [chiral_signs[a // 3] for a in range(12)])


def contract(prop_a, prop_b):
    gammas, chirality = vertex_parts()
    left_real, left_imag, right_real, right_imag = ([], [], [], [])
    for rows_list, phase_list in gammas:
        pick_real = jnp.stack([prop_a[0, q] for q in rows_list])
        pick_imag = jnp.stack([prop_a[1, q] for q in rows_list])
        phase_real = jnp.asarray(np.array([p.real for p in phase_list]), jnp.bfloat16)[
            :, None, None
        ]
        phase_imag = jnp.asarray(np.array([p.imag for p in phase_list]), jnp.bfloat16)[
            :, None, None
        ]
        left_real.append(phase_real * pick_real - phase_imag * pick_imag)
        left_imag.append(phase_real * pick_imag + phase_imag * pick_real)
        col_real = jnp.stack([prop_b[0][:, q] for q in rows_list], axis=1)
        col_imag = jnp.stack([prop_b[1][:, q] for q in rows_list], axis=1)
        factor = np.array(
            [
                [phase_list[c] * chirality[rows_list[c]] * chirality[a] for c in range(12)]
                for a in range(12)
            ]
        )
        factor_real = jnp.asarray(factor.real, jnp.bfloat16)[:, :, None]
        factor_imag = jnp.asarray(factor.imag, jnp.bfloat16)[:, :, None]
        right_real.append(factor_real * col_real + factor_imag * col_imag)
        right_imag.append(factor_imag * col_real - factor_real * col_imag)
    left_rows = jnp.stack(left_real + left_imag).reshape(8, 144, -1)
    right_rows = jnp.stack(right_real + right_imag).reshape(8, 144, -1)
    products = jnp.einsum("mks,nks->mns", left_rows, right_rows, preferred_element_type=jnp.float32)
    real_sum = products[:4, :4] - products[4:, 4:]
    imag_sum = products[:4, 4:] + products[4:, :4]
    return jnp.stack([real_sum.reshape(16, -1), imag_sum.reshape(16, -1)], axis=1)


def dft_tables(length):
    positions = np.arange(length)
    turn_count = positions[:, None] * positions[None, :] % length
    angles = turn_count * (2.0 * math.pi / length)
    cosines = jnp.asarray(np.cos(angles) / math.sqrt(length), jnp.float32)
    sines = jnp.asarray(np.sin(angles) / math.sqrt(length), jnp.float32)
    return (cosines, sines)


def plane_dft(fields):
    cosines, sines = dft_tables(L)
    highest = lax.Precision.HIGHEST
    shape = fields.shape
    grid = fields.reshape(shape[:4] + (L, L))
    real_part = grid[:, :, 0]
    imag_part = grid[:, :, 1]

    def along_z(values, table):
        return jnp.einsum(
            "tfpyz,zk->tfpyk", values, table, precision=highest, preferred_element_type=jnp.float32
        )

    def along_y(values, table):
        return jnp.einsum(
            "tfpyz,yk->tfpkz", values, table, precision=highest, preferred_element_type=jnp.float32
        )

    mid_real = along_z(real_part, cosines) + along_z(imag_part, sines)
    mid_imag = along_z(imag_part, cosines) - along_z(real_part, sines)
    out_real = along_y(mid_real, cosines) + along_y(mid_imag, sines)
    out_imag = along_y(mid_imag, cosines) - along_y(mid_real, sines)
    return jnp.stack([out_real, out_imag], axis=2).reshape(shape)


def line_dft(data):
    length = data.shape[-2]
    cosines, sines = dft_tables(length)
    real_part = data[..., 0, :, :]
    imag_part = data[..., 1, :, :]

    def transform_rows(values, table):
        return jnp.einsum(
            "...xq,xk->...qk",
            values,
            table,
            precision=lax.Precision.HIGHEST,
            preferred_element_type=jnp.float32,
        )

    out_real = transform_rows(real_part, cosines) + transform_rows(imag_part, sines)
    out_imag = transform_rows(imag_part, cosines) - transform_rows(real_part, sines)
    stacked = jnp.stack([out_real, out_imag], axis=-3)
    return stacked.reshape(stacked.shape[:-2] + (stacked.shape[-2] * stacked.shape[-1],))


def on_device(prop_one, prop_two):
    fields = lax.map(
        lambda slice_pair: contract(slice_pair[0], slice_pair[1]), (prop_one, prop_two)
    )
    local_times, field_count, parts, slab = fields.shape
    planes = slab // (L * L)
    fields = plane_dft(fields.reshape(local_times, field_count, parts, planes, L * L))
    turned_fields = line_dft(lax.all_to_all(fields, "xyz", split_axis=4, concat_axis=3, tiled=True))
    result = lax.all_to_all(turned_fields, "ta", split_axis=1, concat_axis=0, tiled=True)
    return result

LANES = 128
GROUP_PERMS = (0, 2)


def spin_tables():
    chi = np.array(chiral_signs)
    alpha = np.array(spin_phases) * chi[None, :]
    beta = np.array([[spin_phases[n][c] * chi[spin_columns[n][c]] for c in range(4)] for n in range(4)])
    groups = []
    for pair, first in enumerate(GROUP_PERMS):
        found = []
        for a in range(4):
            for members in found:
                ratio = alpha[first : first + 2, a] / alpha[first : first + 2, members[0][0]]
                if ratio[0] == ratio[1] and ratio[0] in (1, -1):
                    members.append((a, int(ratio[0].real)))
                    break
            else:
                found.append([(a, 1)])
        assert len(found) == 2
        groups.append(found)
    mixer = np.zeros((2, 4, 4, 2, 2, 2, 2, 16))
    for mu in range(4):
        for nu in range(4):
            for half in range(2):
                lead = groups[mu // 2][half][0][0]
                for row in range(12):
                    m = alpha[mu, lead] * beta[nu, row // 3]
                    at = (mu // 2, half, nu // 2)
                    mixer[(0, mu, nu) + at + (0, row)] = m.real
                    mixer[(0, mu, nu) + at + (1, row)] = -m.imag
                    mixer[(1, mu, nu) + at + (0, row)] = m.imag
                    mixer[(1, mu, nu) + at + (1, row)] = m.real
    return groups, mixer.reshape(32, 256)


def complex_block(table):
    return np.block([[table.real, table.imag], [-table.imag, table.real]])


def high_low(table):
    high = np.asarray(table).astype(jnp.bfloat16)
    low = (table - high.astype(np.float64)).astype(jnp.bfloat16)
    return jnp.asarray(np.stack([high, low]))


def plane_tables(length):
    quarter = LANES // length
    outer = length // quarter
    lane = np.arange(LANES)
    y, z = lane // length, lane % length
    twiddle = np.exp(-2j * np.pi * np.outer(np.arange(outer), y) / length)
    ky, slot = lane // length, lane % length
    kz = (slot % outer) * quarter + slot // outer
    table = np.exp(-2j * np.pi * (np.outer(y, ky) / quarter + np.outer(z, kz) / length)) / length
    return (
        jnp.asarray(np.stack([twiddle.real, twiddle.imag]), jnp.float32),
        high_low(complex_block(table)),
    )


def line_table(length, own, sources):
    x = np.arange(length)
    turn = np.exp(-2j * np.pi * np.outer(x, x) / length) / math.sqrt(length)
    parts = complex_block(turn).reshape(2, sources, length // sources, 2, length)
    full = np.einsum("asxbk,fg->sxafbgk", parts, np.eye(own))
    rows = length * 2 * own
    return high_low(full.reshape(rows, rows))


def split_dot(values, table):
    high = values.astype(jnp.bfloat16)
    low = (values - high.astype(jnp.float32)).astype(jnp.bfloat16)

    def dot(a, b):
        return jnp.dot(a, b, preferred_element_type=jnp.float32)

    return dot(high, table[0]) + (dot(low, table[0]) + dot(high, table[1]))


def small_fft(values):
    count = len(values)
    if count == 1:
        return values
    even, odd = small_fft(values[0::2]), small_fft(values[1::2])
    low, high = [], []
    for k in range(count // 2):
        re, im = odd[k]
        if k == 0:
            pass
        elif 4 * k == count:
            re, im = im, -re
        else:
            c, s = math.cos(2 * math.pi * k / count), math.sin(2 * math.pi * k / count)
            re, im = c * re + s * im, c * im - s * re
        low.append((even[k][0] + re, even[k][1] + im))
        high.append((even[k][0] - re, even[k][1] - im))
    return low + high


def swap_blocks(values):
    width = LANES // 4
    shape = values[0].shape
    block = lax.broadcasted_iota(jnp.int32, shape, len(shape) - 1) // width
    axis = len(shape) - 1
    values = list(values)
    for step in (2, 1):
        keep = (block // step) % 2 == 0
        result = [None] * 4
        for i in range(4):
            if (i // step) % 2 == 0:
                a, b = values[i], values[i + step]
                result[i] = jnp.where(keep, a, pltpu.roll(b, step * width, axis))
                result[i + step] = jnp.where(keep, pltpu.roll(a, LANES - step * width, axis), b)
        values = result
    return values


def partial_sums(tile, zero, groups, one_ref, two_ref, ring, turned, high_ref, low_ref):
    lanes = pl.ds(pl.multiple_of(tile * LANES, LANES), LANES)
    spin = lax.broadcasted_iota(jnp.int32, (12, LANES), 0) // 3
    even = spin % 2 == 0
    for part in range(2):
        for row in range(12):
            value = two_ref[0, part, row, :, lanes].astype(jnp.float32)
            slot = part * 12 + row
            ring[slot, pl.ds(0, 12), :] = value
            ring[slot, pl.ds(zero + 12, 12), :] = value
    for part in range(2):
        for row in range(12):
            slot = part * 12 + row
            third = ring[slot, pl.ds(zero + 9, 12), :]
            first = ring[slot, pl.ds(zero + 3, 12), :]
            turned[0, slot, :, :] = jnp.where(even, third, first)
            turned[1, slot, :, :] = ring[slot, pl.ds(zero + 6, 12), :]
    for pair in range(2):
        columns = spin_columns[GROUP_PERMS[pair]]
        for half in range(2):
            sums = [[None, None], [None, None]]
            for a, sign in groups[pair][half]:
                for colour in range(3):
                    left = columns[a] * 3 + colour
                    right = a * 3 + colour
                    ar = one_ref[0, 0, left, :, lanes].astype(jnp.float32)
                    ai = one_ref[0, 1, left, :, lanes].astype(jnp.float32)
                    for turn in range(2):
                        br = turned[turn, right, :, :]
                        bi = turned[turn, 12 + right, :, :]
                        re = ar * br + ai * bi
                        im = ai * br - ar * bi
                        for at, term in enumerate((re, im)):
                            old = sums[turn][at]
                            if old is None:
                                sums[turn][at] = term
                            elif sign > 0:
                                sums[turn][at] = old + term
                            else:
                                sums[turn][at] = old - term
            for turn in range(2):
                for at in range(2):
                    start = (((pair * 2 + half) * 2 + turn) * 2 + at) * 16
                    total = jnp.concatenate([sums[turn][at], jnp.zeros((4, LANES), jnp.float32)], axis=0)
                    high = total.astype(jnp.bfloat16)
                    high_ref[start : start + 16, lanes] = high
                    low_ref[start : start + 16, lanes] = (total - high.astype(jnp.float32)).astype(jnp.bfloat16)


def plane_blocks(mixer_ref, twiddle_ref, plane_ref, high_ref, low_ref, tiles, store):
    mixer = mixer_ref[...]
    fields = jnp.dot(mixer, high_ref[...], preferred_element_type=jnp.float32) + jnp.dot(
        mixer, low_ref[...], preferred_element_type=jnp.float32
    )
    blocks = [fields[:, t * LANES : (t + 1) * LANES] for t in range(tiles)]
    spectrum = small_fft([(block[:16], block[16:]) for block in blocks])
    turned = []
    for k, (re, im) in enumerate(spectrum):
        c = twiddle_ref[0, k : k + 1, :]
        s = twiddle_ref[1, k : k + 1, :]
        turned.append(jnp.concatenate([re * c - im * s, re * s + im * c], axis=1) if k else jnp.concatenate([re, im], axis=1))
    out = split_dot(jnp.concatenate(turned, axis=0), plane_ref)
    upper = lax.broadcasted_iota(jnp.int32, (8, LANES), 0) < 4
    for half in range(tiles // 4):
        parts = []
        for part in range(2):
            rows = [
                out[(4 * half + p) * 16 : (4 * half + p + 1) * 16, part * LANES : (part + 1) * LANES]
                for p in range(4)
            ]
            parts.append(swap_blocks(rows))
        for k in range(4):
            owner = k * (tiles // 4) + half
            for pair in range(2):
                re = parts[0][k][pair * 8 : pair * 8 + 8]
                im = parts[1][k][pair * 8 : pair * 8 + 8]
                store(owner, 2 * pair, jnp.where(upper, re, pltpu.roll(im, 4, 0)))
                store(owner, 2 * pair + 1, jnp.where(upper, pltpu.roll(re, 4, 0), im))


def finish_time(rows, line_ref, out_ref, at, own):
    out = split_dot(rows.T, line_ref)
    for part in range(2):
        grid = out[:, part * LANES : (part + 1) * LANES].reshape(4, 4, 8, LANES)
        done = swap_blocks([grid[:, q].reshape(32, LANES) for q in range(4)])
        for f in range(own):
            out_ref[at, f, pl.ds(part, 32, stride=2), :] = done[f]


def send_kernel(groups, tiles, one_ref, two_ref, mixer_ref, twiddle_ref, plane_ref, out_ref, ring, turned, high_ref, low_ref):
    zero = jnp.minimum(pl.program_id(0), 0)

    @pl.loop(0, tiles)
    def _(tile):
        partial_sums(tile, zero, groups, one_ref, two_ref, ring, turned, high_ref, low_ref)

    def store(owner, group, value):
        out_ref[owner, group, 0, :, :] = value

    plane_blocks(mixer_ref, twiddle_ref, plane_ref, high_ref, low_ref, tiles, store)


def receive_kernel(times, sources, planes, own, got_ref, line_ref, out_ref):
    for t in range(times):
        rows = got_ref[:, t].reshape(sources * planes * 8, LANES)
        finish_time(rows, line_ref, out_ref, t, own)


def fast_device(prop_one, prop_two, times, sources):
    slab = prop_one.shape[-1]
    plane = L * L
    planes, tiles = slab // plane, plane // LANES
    own = 16 // times
    groups, mixer = spin_tables()
    twiddle, plane_table = plane_tables(L)
    block = pl.BlockSpec((1, 2, 12, 12, plane), lambda x: (0, 0, 0, 0, x))

    def whole(array):
        return pl.BlockSpec(array.shape, lambda x: (0,) * array.ndim)

    mixer = jnp.asarray(mixer, jnp.bfloat16)
    sent = pl.pallas_call(
        lambda *refs: send_kernel(groups, tiles, *refs),
        grid=(planes,),
        out_shape=jax.ShapeDtypeStruct((sources, times, planes, 8, LANES), jnp.float32),
        in_specs=[block, block, whole(mixer), whole(twiddle), whole(plane_table)],
        out_specs=pl.BlockSpec((sources, times, 1, 8, LANES), lambda x: (0, 0, x, 0, 0)),
        scratch_shapes=[
            pltpu.VMEM((24, 24, LANES), jnp.float32),
            pltpu.VMEM((2, 24, 12, LANES), jnp.float32),
            pltpu.VMEM((256, plane), jnp.bfloat16),
            pltpu.VMEM((256, plane), jnp.bfloat16),
        ],
    )(prop_one, prop_two, mixer, twiddle, plane_table)
    got = lax.all_to_all(sent, "xyz", split_axis=0, concat_axis=0, tiled=True)
    got = lax.all_to_all(got, "ta", split_axis=1, concat_axis=1, tiled=True)
    table = line_table(L, own, sources)
    out = pl.pallas_call(
        lambda *refs: receive_kernel(times, sources, planes, own, *refs),
        out_shape=jax.ShapeDtypeStruct((times, own, slab * 2 // LANES, LANES), jnp.float32),
    )(got, table)
    return out.reshape(times, own, slab // LANES, 2, LANES).transpose(0, 1, 3, 2, 4).reshape(times, own, 2, slab)


def solution(mesh):
    placed = (P("ta", None, None, None, "xyz"), P("ta", None, None, None, "xyz"))
    times, sources = mesh.shape["ta"], mesh.shape["xyz"]

    def device(prop_one, prop_two):
        planes = prop_one.shape[-1] // (L * L)
        fits = 4 * L == LANES and planes * sources == L and L // sources == 4 and times == 4
        if fits and prop_one.shape[0] == 1:
            return fast_device(prop_one, prop_two, times, sources)
        return on_device(prop_one, prop_two)

    return jax.shard_map(
        device, mesh=mesh, in_specs=placed, out_specs=P(None, "ta", None, "xyz"), check_vma=False
    )
```

```python
import functools
import math

import jax
import jax.numpy as jnp
import numpy as np
from jax import lax
from jax.experimental import pallas as pl
from jax.experimental.pallas import tpu as pltpu
from jax.sharding import PartitionSpec as P

L = 32


spin_columns = [[3, 2, 1, 0], [3, 2, 1, 0], [2, 3, 0, 1], [2, 3, 0, 1]]
spin_phases = [[1j, 1j, -1j, -1j], [-1.0, 1.0, 1.0, -1.0], [1j, -1j, -1j, 1j], [1.0, 1.0, 1.0, 1.0]]
chiral_signs = [1.0, 1.0, -1.0, -1.0]


def vertex_parts():
    result = []
    for gamma_index in range(4):
        columns = spin_columns[gamma_index]
        phases = spin_phases[gamma_index]
        rows_list = [columns[a // 3] * 3 + a % 3 for a in range(12)]
        phase_list = [complex(phases[a // 3]) for a in range(12)]
        result.append((rows_list, phase_list))
    return (result, [chiral_signs[a // 3] for a in range(12)])


def contract(prop_a, prop_b):
    gammas, chirality = vertex_parts()
    left_real, left_imag, right_real, right_imag = ([], [], [], [])
    for rows_list, phase_list in gammas:
        pick_real = jnp.stack([prop_a[0, q] for q in rows_list])
        pick_imag = jnp.stack([prop_a[1, q] for q in rows_list])
        phase_real = jnp.asarray(np.array([p.real for p in phase_list]), jnp.bfloat16)[
            :, None, None
        ]
        phase_imag = jnp.asarray(np.array([p.imag for p in phase_list]), jnp.bfloat16)[
            :, None, None
        ]
        left_real.append(phase_real * pick_real - phase_imag * pick_imag)
        left_imag.append(phase_real * pick_imag + phase_imag * pick_real)
        col_real = jnp.stack([prop_b[0][:, q] for q in rows_list], axis=1)
        col_imag = jnp.stack([prop_b[1][:, q] for q in rows_list], axis=1)
        factor = np.array(
            [
                [phase_list[c] * chirality[rows_list[c]] * chirality[a] for c in range(12)]
                for a in range(12)
            ]
        )
        factor_real = jnp.asarray(factor.real, jnp.bfloat16)[:, :, None]
        factor_imag = jnp.asarray(factor.imag, jnp.bfloat16)[:, :, None]
        right_real.append(factor_real * col_real + factor_imag * col_imag)
        right_imag.append(factor_imag * col_real - factor_real * col_imag)
    left_rows = jnp.stack(left_real + left_imag).reshape(8, 144, -1)
    right_rows = jnp.stack(right_real + right_imag).reshape(8, 144, -1)
    products = jnp.einsum("mks,nks->mns", left_rows, right_rows, preferred_element_type=jnp.float32)
    real_sum = products[:4, :4] - products[4:, 4:]
    imag_sum = products[:4, 4:] + products[4:, :4]
    return jnp.stack([real_sum.reshape(16, -1), imag_sum.reshape(16, -1)], axis=1)


def dft_tables(length):
    positions = np.arange(length)
    turn_count = positions[:, None] * positions[None, :] % length
    angles = turn_count * (2.0 * math.pi / length)
    cosines = jnp.asarray(np.cos(angles) / math.sqrt(length), jnp.float32)
    sines = jnp.asarray(np.sin(angles) / math.sqrt(length), jnp.float32)
    return (cosines, sines)


def plane_dft(fields):
    cosines, sines = dft_tables(L)
    highest = lax.Precision.HIGHEST
    shape = fields.shape
    grid = fields.reshape(shape[:4] + (L, L))
    real_part = grid[:, :, 0]
    imag_part = grid[:, :, 1]

    def along_z(values, table):
        return jnp.einsum(
            "tfpyz,zk->tfpyk", values, table, precision=highest, preferred_element_type=jnp.float32
        )

    def along_y(values, table):
        return jnp.einsum(
            "tfpyz,yk->tfpkz", values, table, precision=highest, preferred_element_type=jnp.float32
        )

    mid_real = along_z(real_part, cosines) + along_z(imag_part, sines)
    mid_imag = along_z(imag_part, cosines) - along_z(real_part, sines)
    out_real = along_y(mid_real, cosines) + along_y(mid_imag, sines)
    out_imag = along_y(mid_imag, cosines) - along_y(mid_real, sines)
    return jnp.stack([out_real, out_imag], axis=2).reshape(shape)


def line_dft(data):
    length = data.shape[-2]
    cosines, sines = dft_tables(length)
    real_part = data[..., 0, :, :]
    imag_part = data[..., 1, :, :]

    def transform_rows(values, table):
        return jnp.einsum(
            "...xq,xk->...qk",
            values,
            table,
            precision=lax.Precision.HIGHEST,
            preferred_element_type=jnp.float32,
        )

    out_real = transform_rows(real_part, cosines) + transform_rows(imag_part, sines)
    out_imag = transform_rows(imag_part, cosines) - transform_rows(real_part, sines)
    stacked = jnp.stack([out_real, out_imag], axis=-3)
    return stacked.reshape(stacked.shape[:-2] + (stacked.shape[-2] * stacked.shape[-1],))


def on_device(prop_one, prop_two):
    fields = lax.map(
        lambda slice_pair: contract(slice_pair[0], slice_pair[1]), (prop_one, prop_two)
    )
    local_times, field_count, parts, slab = fields.shape
    planes = slab // (L * L)
    fields = plane_dft(fields.reshape(local_times, field_count, parts, planes, L * L))
    turned_fields = line_dft(lax.all_to_all(fields, "xyz", split_axis=4, concat_axis=3, tiled=True))
    result = lax.all_to_all(turned_fields, "ta", split_axis=1, concat_axis=0, tiled=True)
    return result

LANES = 128
GROUP_PERMS = (0, 2)


def spin_tables():
    chi = np.array(chiral_signs)
    alpha = np.array(spin_phases) * chi[None, :]
    beta = np.array([[spin_phases[n][c] * chi[spin_columns[n][c]] for c in range(4)] for n in range(4)])
    tables = []
    for phases in (alpha, beta):
        pairs = []
        for first in GROUP_PERMS:
            found = []
            for a in range(4):
                for members in found:
                    ratio = phases[first : first + 2, a] / phases[first : first + 2, members[0][0]]
                    if ratio[0] == ratio[1] and ratio[0] in (1, -1):
                        members.append((a, int(ratio[0].real)))
                        break
                else:
                    found.append([(a, 1)])
            assert len(found) == 2
            pairs.append(found)
        lead = np.array([[phases[m, pairs[m // 2][half][0][0]] for half in range(2)] for m in range(4)])
        signs = np.array([[int((lead[m, half] / lead[m, 0]).real) for half in range(2)] for m in range(4)])
        tables.append((pairs, lead[:, 0], signs))
    left, right = tables
    phase = np.outer(left[1], right[1]).reshape(16)
    return left[0], left[2], right[0], right[2], phase


def complex_block(table):
    return np.block([[table.real, table.imag], [-table.imag, table.real]])


def high_low(table):
    high = np.asarray(table).astype(jnp.bfloat16)
    low = (table - high.astype(np.float64)).astype(jnp.bfloat16)
    return jnp.asarray(np.stack([high, low]))


def plane_tables(length):
    quarter = LANES // length
    outer = length // quarter
    lane = np.arange(LANES)
    y, z = lane // length, lane % length
    twiddle = np.exp(-2j * np.pi * np.outer(np.arange(outer), y) / length)
    ky, slot = lane // length, lane % length
    kz = (slot % outer) * quarter + slot // outer
    table = np.exp(-2j * np.pi * (np.outer(y, ky) / quarter + np.outer(z, kz) / length)) / length
    return (
        jnp.asarray(np.stack([twiddle.real, twiddle.imag]), jnp.float32),
        high_low(complex_block(table)),
    )


def line_table(length, own, sources):
    x = np.arange(length)
    turn = np.exp(-2j * np.pi * np.outer(x, x) / length) / math.sqrt(length)
    parts = complex_block(turn).reshape(2, sources, length // sources, 2, length)
    full = np.einsum("asxbk,fg->sxafbgk", parts, np.eye(own))
    rows = length * 2 * own
    return high_low(full.reshape(rows, rows))


def split_dot(values, table):
    high = values.astype(jnp.bfloat16)
    low = (values - high.astype(jnp.float32)).astype(jnp.bfloat16)

    def dot(a, b):
        return jnp.dot(a, b, preferred_element_type=jnp.float32)

    return dot(high, table[0]) + (dot(low, table[0]) + dot(high, table[1]))


def small_fft(values):
    count = len(values)
    if count == 1:
        return values
    even, odd = small_fft(values[0::2]), small_fft(values[1::2])
    low, high = [], []
    for k in range(count // 2):
        re, im = odd[k]
        if k == 0:
            pass
        elif 4 * k == count:
            re, im = im, -re
        else:
            c, s = math.cos(2 * math.pi * k / count), math.sin(2 * math.pi * k / count)
            re, im = c * re + s * im, c * im - s * re
        low.append((even[k][0] + re, even[k][1] + im))
        high.append((even[k][0] - re, even[k][1] - im))
    return low + high


def swap_blocks(values):
    width = LANES // 4
    shape = values[0].shape
    block = lax.broadcasted_iota(jnp.int32, shape, len(shape) - 1) // width
    axis = len(shape) - 1
    values = list(values)
    for step in (2, 1):
        keep = (block // step) % 2 == 0
        result = [None] * 4
        for i in range(4):
            if (i // step) % 2 == 0:
                a, b = values[i], values[i + step]
                result[i] = jnp.where(keep, a, pltpu.roll(b, step * width, axis))
                result[i + step] = jnp.where(keep, pltpu.roll(a, LANES - step * width, axis), b)
        values = result
    return values


def add_signed(total, term, sign):
    if total is None:
        return term if sign > 0 else -term
    return total + term if sign > 0 else total - term


def site_sums(tables, one_ref, two_ref, wide, turned, mixed):
    left_groups, left_signs, right_groups, right_signs, _ = tables
    rows = one_ref.shape[2]
    even = lax.broadcasted_iota(jnp.int32, (8, LANES), 0) % 2 == 0

    @pl.loop(0, 12)
    def _(a):
        for c in range(12):
            value = two_ref[a, c, :, :].astype(jnp.float32)
            wide[a, c, :, :] = value
            for at in range(0, rows, 8):
                piece = value[at : at + 8]
                turned[a, c, at : at + 8, :] = jnp.where(even, pltpu.roll(piece, 7, 0), pltpu.roll(piece, 1, 0))

    for pair in range(2):
        left_columns = spin_columns[GROUP_PERMS[pair]]
        sums = {}
        for half in range(2):
            for turn in range(2):
                right_columns = spin_columns[GROUP_PERMS[turn]]
                for side in range(2):
                    straight, crossed = None, None
                    for a, left_sign in left_groups[pair][half]:
                        for c, right_sign in right_groups[turn][side]:
                            for i in range(3):
                                for j in range(3):
                                    sink, source = left_columns[a] * 3 + i, c * 3 + j
                                    first = one_ref[sink, source, :, :].astype(jnp.float32)
                                    at = (a * 3 + i, right_columns[c] * 3 + j)
                                    sign = left_sign * right_sign
                                    straight = add_signed(straight, first * wide[at[0], at[1], :, :], sign)
                                    crossed = add_signed(crossed, first * turned[at[0], at[1], :, :], sign)
                    sums[half, turn, side] = (straight, crossed)
        for mu in (2 * pair, 2 * pair + 1):
            for nu in range(4):
                for kind in range(2):
                    total = None
                    for half in range(2):
                        for side in range(2):
                            sign = int(left_signs[mu][half] * right_signs[nu][side])
                            total = add_signed(total, sums[half, nu // 2, side][kind], sign)
                    start = (4 * mu + nu) * rows
                    mixed[kind, start : start + rows, :] = total


def plane_blocks(phase_ref, twiddle_ref, plane_ref, mixed, tiles, store):
    blocks = []
    for t in range(tiles):
        straight = [mixed[0, pl.ds(2 * t + part, 16, stride=2 * tiles), :] for part in range(2)]
        crossed = [mixed[1, pl.ds(2 * t + part, 16, stride=2 * tiles), :] for part in range(2)]
        re, im = straight[0] + straight[1], crossed[1] - crossed[0]
        c, s = phase_ref[0], phase_ref[1]
        blocks.append((c * re - s * im, c * im + s * re))
    spectrum = small_fft(blocks)
    turned = []
    for k, (re, im) in enumerate(spectrum):
        c = twiddle_ref[0, k : k + 1, :]
        s = twiddle_ref[1, k : k + 1, :]
        turned.append(jnp.concatenate([re * c - im * s, re * s + im * c], axis=1) if k else jnp.concatenate([re, im], axis=1))
    out = split_dot(jnp.concatenate(turned, axis=0), plane_ref)
    upper = lax.broadcasted_iota(jnp.int32, (8, LANES), 0) < 4
    for half in range(tiles // 4):
        parts = []
        for part in range(2):
            rows = [
                out[(4 * half + p) * 16 : (4 * half + p + 1) * 16, part * LANES : (part + 1) * LANES]
                for p in range(4)
            ]
            parts.append(swap_blocks(rows))
        for k in range(4):
            owner = k * (tiles // 4) + half
            for pair in range(2):
                re = parts[0][k][pair * 8 : pair * 8 + 8]
                im = parts[1][k][pair * 8 : pair * 8 + 8]
                store(owner, 2 * pair, jnp.where(upper, re, pltpu.roll(im, 4, 0)))
                store(owner, 2 * pair + 1, jnp.where(upper, pltpu.roll(re, 4, 0), im))


def finish_time(rows, line_ref, out_ref, at, own):
    out = split_dot(rows.T, line_ref)
    for part in range(2):
        grid = out[:, part * LANES : (part + 1) * LANES].reshape(4, 4, 8, LANES)
        done = swap_blocks([grid[:, q].reshape(32, LANES) for q in range(4)])
        for f in range(own):
            out_ref[at, f, pl.ds(part, 32, stride=2), :] = done[f]


def fused_kernel(
    tables, tiles, planes, times, sources, own, names,
    one_ref, two_ref, phase_ref, twiddle_ref, plane_ref, line_ref, out_ref,
    wide, turned, mixed, send, got, send_sem, recv_sem,
):
    step = pl.program_id(0)
    t, s = lax.axis_index(names[0]), lax.axis_index(names[1])
    far = sorted(range(sources), key=lambda o: -min(o, sources - o))
    offsets = [(a, o) for o in far for a in reversed(range(times)) if (a, o) != (0, 0)]
    barrier = pltpu.get_barrier_semaphore()

    def peer(a, o):
        return lax.rem(t + a, times), lax.rem(s + o, sources)

    def copy(x, k):
        to_t, to_s = peer(*offsets[k])
        return pltpu.make_async_remote_copy(
            src_ref=send.at[to_s, to_t, x],
            dst_ref=got.at[t, s, x],
            send_sem=send_sem.at[x, k],
            recv_sem=recv_sem.at[x, k],
            device_id={names[0]: to_t, names[1]: to_s},
            device_id_type=pl.DeviceIdType.MESH,
        )

    def arrival(x, k):
        a, o = offsets[k]
        from_t, from_s = peer(times - a, sources - o)
        return pltpu.make_async_remote_copy(
            src_ref=send.at[from_s, from_t, x],
            dst_ref=got.at[from_t, from_s, x],
            send_sem=send_sem.at[x, k],
            recv_sem=recv_sem.at[x, k],
            device_id={names[0]: from_t, names[1]: from_s},
            device_id_type=pl.DeviceIdType.MESH,
        )

    @pl.when(step == 0)
    def _():
        for a, o in offsets:
            to_t, to_s = peer(a, o)
            pl.semaphore_signal(
                barrier, inc=1, device_id={names[0]: to_t, names[1]: to_s}, device_id_type=pl.DeviceIdType.MESH
            )

    site_sums(tables, one_ref, two_ref, wide, turned, mixed)

    def store(owner, group, value):
        send[owner, group, step, :, :] = value

    plane_blocks(phase_ref, twiddle_ref, plane_ref, mixed, tiles, store)

    @pl.when(step == 0)
    def _():
        pl.semaphore_wait(barrier, len(offsets))

    for k in range(len(offsets)):
        copy(step, k).start()
    got[t, s, step, :, :] = send[s, t, step, :, :]

    @pl.when(step == planes - 1)
    def _():
        for a in range(times):
            @pl.loop(0, planes)
            def _(x):
                for k in range(len(offsets)):
                    if offsets[k][0] == a:
                        arrival(x, k).wait_recv()
                        copy(x, k).wait_send()
            from_t = lax.rem(t + times - a, times)
            rows = got[from_t].reshape(sources * planes * 8, LANES)
            finish_time(rows, line_ref, out_ref, from_t, own)


def fast_device(prop_one, prop_two, times, sources):
    slab = prop_one.shape[-1]
    plane = L * L
    planes, tiles = slab // plane, plane // LANES
    own = 16 // times
    tables = spin_tables()
    twiddle, plane_table = plane_tables(L)
    line = line_table(L, own, sources)
    phase = np.broadcast_to(tables[4][:, None], (16, LANES))
    phase = jnp.asarray(np.stack([phase.real, phase.imag]), jnp.float32)

    def paired(prop):
        split = prop.reshape(2, 12, 12, slab // LANES, LANES).transpose(1, 2, 3, 0, 4)
        return split.reshape(12, 12, slab // LANES * 2, LANES)

    block = pl.BlockSpec((12, 12, 2 * tiles, LANES), lambda x: (0, 0, x, 0))

    def whole(shape):
        return pl.BlockSpec(shape, lambda x: (0,) * len(shape))

    peers = times * sources - 1
    shape = (times, own, slab * 2 // LANES, LANES)
    out = pl.pallas_call(
        functools.partial(fused_kernel, tables, tiles, planes, times, sources, own, ("ta", "xyz")),
        grid=(planes,),
        out_shape=jax.ShapeDtypeStruct(shape, jnp.float32),
        in_specs=[block, block] + [whole(v.shape) for v in (phase, twiddle, plane_table, line)],
        out_specs=whole(shape),
        scratch_shapes=[
            pltpu.VMEM((12, 12, 2 * tiles, LANES), jnp.float32),
            pltpu.VMEM((12, 12, 2 * tiles, LANES), jnp.float32),
            pltpu.VMEM((2, 16 * 2 * tiles, LANES), jnp.float32),
            pltpu.VMEM((sources, times, planes, 8, LANES), jnp.float32),
            pltpu.VMEM((times, sources, planes, 8, LANES), jnp.float32),
            pltpu.SemaphoreType.DMA((planes, peers)),
            pltpu.SemaphoreType.DMA((planes, peers)),
        ],
        compiler_params=pltpu.CompilerParams(
            collective_id=0, has_side_effects=True, dimension_semantics=("arbitrary",)
        ),
    )(paired(prop_one), paired(prop_two), phase, twiddle, plane_table, line)
    return out.reshape(times, own, slab // LANES, 2, LANES).transpose(0, 1, 3, 2, 4).reshape(times, own, 2, slab)


def solution(mesh):
    placed = (P("ta", None, None, None, "xyz"), P("ta", None, None, None, "xyz"))
    times, sources = mesh.shape["ta"], mesh.shape["xyz"]

    def device(prop_one, prop_two):
        planes = prop_one.shape[-1] // (L * L)
        fits = 4 * L == LANES and planes * sources == L and L // sources == 4 and times == 4
        if fits and prop_one.shape[0] == 1:
            return fast_device(prop_one, prop_two, times, sources)
        return on_device(prop_one, prop_two)

    return jax.shard_map(
        device, mesh=mesh, in_specs=placed, out_specs=P(None, "ta", None, "xyz"), check_vma=False
    )
```

```python
import functools
import math

import jax
import jax.numpy as jnp
import numpy as np
from jax import lax
from jax.experimental import pallas as pl
from jax.experimental.pallas import tpu as pltpu
from jax.sharding import PartitionSpec as P

L = 32


spin_columns = [[3, 2, 1, 0], [3, 2, 1, 0], [2, 3, 0, 1], [2, 3, 0, 1]]
spin_phases = [[1j, 1j, -1j, -1j], [-1.0, 1.0, 1.0, -1.0], [1j, -1j, -1j, 1j], [1.0, 1.0, 1.0, 1.0]]
chiral_signs = [1.0, 1.0, -1.0, -1.0]


def vertex_parts():
    result = []
    for gamma_index in range(4):
        columns = spin_columns[gamma_index]
        phases = spin_phases[gamma_index]
        rows_list = [columns[a // 3] * 3 + a % 3 for a in range(12)]
        phase_list = [complex(phases[a // 3]) for a in range(12)]
        result.append((rows_list, phase_list))
    return (result, [chiral_signs[a // 3] for a in range(12)])


def contract(prop_a, prop_b):
    gammas, chirality = vertex_parts()
    left_real, left_imag, right_real, right_imag = ([], [], [], [])
    for rows_list, phase_list in gammas:
        pick_real = jnp.stack([prop_a[0, q] for q in rows_list])
        pick_imag = jnp.stack([prop_a[1, q] for q in rows_list])
        phase_real = jnp.asarray(np.array([p.real for p in phase_list]), jnp.bfloat16)[
            :, None, None
        ]
        phase_imag = jnp.asarray(np.array([p.imag for p in phase_list]), jnp.bfloat16)[
            :, None, None
        ]
        left_real.append(phase_real * pick_real - phase_imag * pick_imag)
        left_imag.append(phase_real * pick_imag + phase_imag * pick_real)
        col_real = jnp.stack([prop_b[0][:, q] for q in rows_list], axis=1)
        col_imag = jnp.stack([prop_b[1][:, q] for q in rows_list], axis=1)
        factor = np.array(
            [
                [phase_list[c] * chirality[rows_list[c]] * chirality[a] for c in range(12)]
                for a in range(12)
            ]
        )
        factor_real = jnp.asarray(factor.real, jnp.bfloat16)[:, :, None]
        factor_imag = jnp.asarray(factor.imag, jnp.bfloat16)[:, :, None]
        right_real.append(factor_real * col_real + factor_imag * col_imag)
        right_imag.append(factor_imag * col_real - factor_real * col_imag)
    left_rows = jnp.stack(left_real + left_imag).reshape(8, 144, -1)
    right_rows = jnp.stack(right_real + right_imag).reshape(8, 144, -1)
    products = jnp.einsum("mks,nks->mns", left_rows, right_rows, preferred_element_type=jnp.float32)
    real_sum = products[:4, :4] - products[4:, 4:]
    imag_sum = products[:4, 4:] + products[4:, :4]
    return jnp.stack([real_sum.reshape(16, -1), imag_sum.reshape(16, -1)], axis=1)


def dft_tables(length):
    positions = np.arange(length)
    turn_count = positions[:, None] * positions[None, :] % length
    angles = turn_count * (2.0 * math.pi / length)
    cosines = jnp.asarray(np.cos(angles) / math.sqrt(length), jnp.float32)
    sines = jnp.asarray(np.sin(angles) / math.sqrt(length), jnp.float32)
    return (cosines, sines)


def plane_dft(fields):
    cosines, sines = dft_tables(L)
    highest = lax.Precision.HIGHEST
    shape = fields.shape
    grid = fields.reshape(shape[:4] + (L, L))
    real_part = grid[:, :, 0]
    imag_part = grid[:, :, 1]

    def along_z(values, table):
        return jnp.einsum(
            "tfpyz,zk->tfpyk", values, table, precision=highest, preferred_element_type=jnp.float32
        )

    def along_y(values, table):
        return jnp.einsum(
            "tfpyz,yk->tfpkz", values, table, precision=highest, preferred_element_type=jnp.float32
        )

    mid_real = along_z(real_part, cosines) + along_z(imag_part, sines)
    mid_imag = along_z(imag_part, cosines) - along_z(real_part, sines)
    out_real = along_y(mid_real, cosines) + along_y(mid_imag, sines)
    out_imag = along_y(mid_imag, cosines) - along_y(mid_real, sines)
    return jnp.stack([out_real, out_imag], axis=2).reshape(shape)


def line_dft(data):
    length = data.shape[-2]
    cosines, sines = dft_tables(length)
    real_part = data[..., 0, :, :]
    imag_part = data[..., 1, :, :]

    def transform_rows(values, table):
        return jnp.einsum(
            "...xq,xk->...qk",
            values,
            table,
            precision=lax.Precision.HIGHEST,
            preferred_element_type=jnp.float32,
        )

    out_real = transform_rows(real_part, cosines) + transform_rows(imag_part, sines)
    out_imag = transform_rows(imag_part, cosines) - transform_rows(real_part, sines)
    stacked = jnp.stack([out_real, out_imag], axis=-3)
    return stacked.reshape(stacked.shape[:-2] + (stacked.shape[-2] * stacked.shape[-1],))


def on_device(prop_one, prop_two):
    fields = lax.map(
        lambda slice_pair: contract(slice_pair[0], slice_pair[1]), (prop_one, prop_two)
    )
    local_times, field_count, parts, slab = fields.shape
    planes = slab // (L * L)
    fields = plane_dft(fields.reshape(local_times, field_count, parts, planes, L * L))
    turned_fields = line_dft(lax.all_to_all(fields, "xyz", split_axis=4, concat_axis=3, tiled=True))
    result = lax.all_to_all(turned_fields, "ta", split_axis=1, concat_axis=0, tiled=True)
    return result

LANES = 128
GROUP_PERMS = (0, 2)


def spin_tables():
    chi = np.array(chiral_signs)
    alpha = np.array(spin_phases) * chi[None, :]
    beta = np.array([[spin_phases[n][c] * chi[spin_columns[n][c]] for c in range(4)] for n in range(4)])
    tables = []
    for phases in (alpha, beta):
        pairs = []
        for first in GROUP_PERMS:
            found = []
            for a in range(4):
                for members in found:
                    ratio = phases[first : first + 2, a] / phases[first : first + 2, members[0][0]]
                    if ratio[0] == ratio[1] and ratio[0] in (1, -1):
                        members.append((a, int(ratio[0].real)))
                        break
                else:
                    found.append([(a, 1)])
            assert len(found) == 2
            pairs.append(found)
        lead = np.array([[phases[m, pairs[m // 2][half][0][0]] for half in range(2)] for m in range(4)])
        signs = np.array([[int((lead[m, half] / lead[m, 0]).real) for half in range(2)] for m in range(4)])
        tables.append((pairs, lead[:, 0], signs))
    left, right = tables
    phase = np.outer(left[1], right[1]).reshape(16)
    return left[0], left[2], right[0], right[2], phase


def complex_block(table):
    return np.block([[table.real, table.imag], [-table.imag, table.real]])


def high_low(table):
    high = np.asarray(table).astype(jnp.bfloat16)
    low = (table - high.astype(np.float64)).astype(jnp.bfloat16)
    return jnp.asarray(np.stack([high, low]))


def plane_tables(length):
    quarter = LANES // length
    outer = length // quarter
    lane = np.arange(LANES)
    y, z = lane // length, lane % length
    twiddle = np.exp(-2j * np.pi * np.outer(np.arange(outer), y) / length)
    ky, slot = lane // length, lane % length
    kz = (slot % outer) * quarter + slot // outer
    table = np.exp(-2j * np.pi * (np.outer(y, ky) / quarter + np.outer(z, kz) / length)) / length
    return (
        jnp.asarray(np.stack([twiddle.real, twiddle.imag]), jnp.float32),
        high_low(complex_block(table)),
    )


def line_table(length, own, sources):
    x = np.arange(length)
    turn = np.exp(-2j * np.pi * np.outer(x, x) / length) / math.sqrt(length)
    parts = complex_block(turn).reshape(2, sources, length // sources, 2, length)
    full = np.einsum("asxbk,fg->sxafbgk", parts, np.eye(own))
    rows = length * 2 * own
    return high_low(full.reshape(rows, rows))


def split_dot(values, table):
    high = values.astype(jnp.bfloat16)
    low = (values - high.astype(jnp.float32)).astype(jnp.bfloat16)

    def dot(a, b):
        return jnp.dot(a, b, preferred_element_type=jnp.float32)

    return dot(high, table[0]) + (dot(low, table[0]) + dot(high, table[1]))


def small_fft(values):
    count = len(values)
    if count == 1:
        return values
    even, odd = small_fft(values[0::2]), small_fft(values[1::2])
    low, high = [], []
    for k in range(count // 2):
        re, im = odd[k]
        if k == 0:
            pass
        elif 4 * k == count:
            re, im = im, -re
        else:
            c, s = math.cos(2 * math.pi * k / count), math.sin(2 * math.pi * k / count)
            re, im = c * re + s * im, c * im - s * re
        low.append((even[k][0] + re, even[k][1] + im))
        high.append((even[k][0] - re, even[k][1] - im))
    return low + high


def swap_blocks(values):
    width = LANES // 4
    shape = values[0].shape
    block = lax.broadcasted_iota(jnp.int32, shape, len(shape) - 1) // width
    axis = len(shape) - 1
    values = list(values)
    for step in (2, 1):
        keep = (block // step) % 2 == 0
        result = [None] * 4
        for i in range(4):
            if (i // step) % 2 == 0:
                a, b = values[i], values[i + step]
                result[i] = jnp.where(keep, a, pltpu.roll(b, step * width, axis))
                result[i + step] = jnp.where(keep, pltpu.roll(a, LANES - step * width, axis), b)
        values = result
    return values


def add_signed(total, term, sign):
    if total is None:
        return term if sign > 0 else -term
    return total + term if sign > 0 else total - term


def site_sums(tables, one_ref, two_ref, wide, turned, mixed):
    left_groups, left_signs, right_groups, right_signs, _ = tables
    rows = one_ref.shape[2]
    even = lax.broadcasted_iota(jnp.int32, (8, LANES), 0) % 2 == 0

    @pl.loop(0, 12)
    def _(a):
        for c in range(12):
            value = two_ref[a, c, :, :].astype(jnp.float32)
            wide[a, c, :, :] = value
            for at in range(0, rows, 8):
                piece = value[at : at + 8]
                turned[a, c, at : at + 8, :] = jnp.where(even, pltpu.roll(piece, 7, 0), pltpu.roll(piece, 1, 0))

    for pair in range(2):
        left_columns = spin_columns[GROUP_PERMS[pair]]
        sums = {}
        for half in range(2):
            for turn in range(2):
                right_columns = spin_columns[GROUP_PERMS[turn]]
                for side in range(2):
                    straight, crossed = None, None
                    for a, left_sign in left_groups[pair][half]:
                        for c, right_sign in right_groups[turn][side]:
                            for i in range(3):
                                for j in range(3):
                                    sink, source = left_columns[a] * 3 + i, c * 3 + j
                                    first = one_ref[sink, source, :, :].astype(jnp.float32)
                                    at = (a * 3 + i, right_columns[c] * 3 + j)
                                    sign = left_sign * right_sign
                                    straight = add_signed(straight, first * wide[at[0], at[1], :, :], sign)
                                    crossed = add_signed(crossed, first * turned[at[0], at[1], :, :], sign)
                    sums[half, turn, side] = (straight, crossed)
        for mu in (2 * pair, 2 * pair + 1):
            for nu in range(4):
                for kind in range(2):
                    total = None
                    for half in range(2):
                        for side in range(2):
                            sign = int(left_signs[mu][half] * right_signs[nu][side])
                            total = add_signed(total, sums[half, nu // 2, side][kind], sign)
                    start = (4 * mu + nu) * rows
                    mixed[kind, start : start + rows, :] = total


def plane_blocks(phase_ref, twiddle_ref, plane_ref, mixed, tiles, store):
    blocks = []
    for t in range(tiles):
        straight = [mixed[0, pl.ds(2 * t + part, 16, stride=2 * tiles), :] for part in range(2)]
        crossed = [mixed[1, pl.ds(2 * t + part, 16, stride=2 * tiles), :] for part in range(2)]
        re, im = straight[0] + straight[1], crossed[1] - crossed[0]
        c, s = phase_ref[0], phase_ref[1]
        blocks.append((c * re - s * im, c * im + s * re))
    spectrum = small_fft(blocks)
    turned = []
    for k, (re, im) in enumerate(spectrum):
        c = twiddle_ref[0, k : k + 1, :]
        s = twiddle_ref[1, k : k + 1, :]
        turned.append(jnp.concatenate([re * c - im * s, re * s + im * c], axis=1) if k else jnp.concatenate([re, im], axis=1))
    out = split_dot(jnp.concatenate(turned, axis=0), plane_ref)
    upper = lax.broadcasted_iota(jnp.int32, (8, LANES), 0) < 4
    for half in range(tiles // 4):
        parts = []
        for part in range(2):
            rows = [
                out[(4 * half + p) * 16 : (4 * half + p + 1) * 16, part * LANES : (part + 1) * LANES]
                for p in range(4)
            ]
            parts.append(swap_blocks(rows))
        for k in range(4):
            owner = k * (tiles // 4) + half
            for pair in range(2):
                re = parts[0][k][pair * 8 : pair * 8 + 8]
                im = parts[1][k][pair * 8 : pair * 8 + 8]
                store(owner, 2 * pair, jnp.where(upper, re, pltpu.roll(im, 4, 0)))
                store(owner, 2 * pair + 1, jnp.where(upper, pltpu.roll(re, 4, 0), im))


def finish_time(rows, line_ref, out_ref, at, own):
    out = split_dot(rows.T, line_ref)
    for part in range(2):
        grid = out[:, part * LANES : (part + 1) * LANES].reshape(4, 4, 8, LANES)
        done = swap_blocks([grid[:, q].reshape(32, LANES) for q in range(4)])
        for f in range(own):
            out_ref[at, f, pl.ds(part, 32, stride=2), :] = done[f]


def fused_kernel(
    tables, tiles, planes, times, sources, own, names,
    one_ref, two_ref, phase_ref, twiddle_ref, plane_ref, line_ref, out_ref,
    wide, turned, mixed, send, got, send_sem, recv_sem,
):
    step = pl.program_id(0)
    t, s = lax.axis_index(names[0]), lax.axis_index(names[1])
    far = sorted(range(sources), key=lambda o: -min(o, sources - o))
    offsets = [(a, o) for a in range(times) for o in far if (a, o) != (0, 0)]
    barrier = pltpu.get_barrier_semaphore()

    def peer(a, o):
        return lax.rem(t + a, times), lax.rem(s + o, sources)

    def copy(k):
        to_t, to_s = peer(*offsets[k])
        return pltpu.make_async_remote_copy(
            src_ref=send.at[to_s, to_t],
            dst_ref=got.at[t, s],
            send_sem=send_sem.at[k],
            recv_sem=recv_sem.at[k],
            device_id={names[0]: to_t, names[1]: to_s},
            device_id_type=pl.DeviceIdType.MESH,
        )

    def arrival(k):
        a, o = offsets[k]
        from_t, from_s = peer(times - a, sources - o)
        return pltpu.make_async_remote_copy(
            src_ref=send.at[from_s, from_t],
            dst_ref=got.at[from_t, from_s],
            send_sem=send_sem.at[k],
            recv_sem=recv_sem.at[k],
            device_id={names[0]: from_t, names[1]: from_s},
            device_id_type=pl.DeviceIdType.MESH,
        )

    @pl.when(step == 0)
    def _():
        for a, o in offsets:
            to_t, to_s = peer(a, o)
            pl.semaphore_signal(
                barrier, inc=1, device_id={names[0]: to_t, names[1]: to_s}, device_id_type=pl.DeviceIdType.MESH
            )

    site_sums(tables, one_ref, two_ref, wide, turned, mixed)

    def store(owner, group, value):
        send[owner, group, step, :, :] = value

    plane_blocks(phase_ref, twiddle_ref, plane_ref, mixed, tiles, store)

    @pl.when(step == planes - 1)
    def _():
        pl.semaphore_wait(barrier, len(offsets))
        for k in range(len(offsets)):
            copy(k).start()
        got[t, s, :, :, :] = send[s, t, :, :, :]
        for a in range(times):
            for k in range(len(offsets)):
                if offsets[k][0] == a:
                    arrival(k).wait_recv()
            from_t = lax.rem(t + times - a, times)
            rows = got[from_t].reshape(sources * planes * 8, LANES)
            finish_time(rows, line_ref, out_ref, from_t, own)
        for k in range(len(offsets)):
            copy(k).wait_send()


def fast_device(prop_one, prop_two, times, sources):
    slab = prop_one.shape[-1]
    plane = L * L
    planes, tiles = slab // plane, plane // LANES
    own = 16 // times
    tables = spin_tables()
    twiddle, plane_table = plane_tables(L)
    line = line_table(L, own, sources)
    phase = np.broadcast_to(tables[4][:, None], (16, LANES))
    phase = jnp.asarray(np.stack([phase.real, phase.imag]), jnp.float32)

    def paired(prop):
        split = prop.reshape(2, 12, 12, slab // LANES, LANES).transpose(1, 2, 3, 0, 4)
        return split.reshape(12, 12, slab // LANES * 2, LANES)

    block = pl.BlockSpec((12, 12, 2 * tiles, LANES), lambda x: (0, 0, x, 0))

    def whole(shape):
        return pl.BlockSpec(shape, lambda x: (0,) * len(shape))

    peers = times * sources - 1
    shape = (times, own, slab * 2 // LANES, LANES)
    out = pl.pallas_call(
        functools.partial(fused_kernel, tables, tiles, planes, times, sources, own, ("ta", "xyz")),
        grid=(planes,),
        out_shape=jax.ShapeDtypeStruct(shape, jnp.float32),
        in_specs=[block, block] + [whole(v.shape) for v in (phase, twiddle, plane_table, line)],
        out_specs=whole(shape),
        scratch_shapes=[
            pltpu.VMEM((12, 12, 2 * tiles, LANES), jnp.float32),
            pltpu.VMEM((12, 12, 2 * tiles, LANES), jnp.float32),
            pltpu.VMEM((2, 16 * 2 * tiles, LANES), jnp.float32),
            pltpu.VMEM((sources, times, planes, 8, LANES), jnp.float32),
            pltpu.VMEM((times, sources, planes, 8, LANES), jnp.float32),
            pltpu.SemaphoreType.DMA((peers,)),
            pltpu.SemaphoreType.DMA((peers,)),
        ],
        compiler_params=pltpu.CompilerParams(
            collective_id=0, has_side_effects=True, dimension_semantics=("arbitrary",)
        ),
    )(paired(prop_one), paired(prop_two), phase, twiddle, plane_table, line)
    return out.reshape(times, own, slab // LANES, 2, LANES).transpose(0, 1, 3, 2, 4).reshape(times, own, 2, slab)


def solution(mesh):
    placed = (P("ta", None, None, None, "xyz"), P("ta", None, None, None, "xyz"))
    times, sources = mesh.shape["ta"], mesh.shape["xyz"]

    def device(prop_one, prop_two):
        planes = prop_one.shape[-1] // (L * L)
        fits = 4 * L == LANES and planes * sources == L and L // sources == 4 and times == 4
        if fits and prop_one.shape[0] == 1:
            return fast_device(prop_one, prop_two, times, sources)
        return on_device(prop_one, prop_two)

    return jax.shard_map(
        device, mesh=mesh, in_specs=placed, out_specs=P(None, "ta", None, "xyz"), check_vma=False
    )
```
